32 devices in a mesh: gx: 8 (over y, x, core), gy: 4 (over z).
Axes of the slice: x: 2, y: 2, z: 4, core: 2. Of those that a mesh axis runs over, the one named last changes fastest.
Arguments:
- spectrum: float32 [192, 160, 1080], P('gx', 'gy'), may hold values from 0.05 to 1
- adjoint_in: float32 [192, 160, 1080], P('gx', 'gy'), may hold values from 0 to 2
- current_x: float32 [192, 160], P('gx', 'gy'), may hold values from -0.08 to 0.08
- current_y: float32 [192, 160], P('gx', 'gy'), may hold values from -0.08 to 0.08
- wind_x: float32 [192, 160], P('gx', 'gy'), may hold values from -4 to 4
- wind_y: float32 [192, 160], P('gx', 'gy'), may hold values from -4 to 4
- land_mask: int32 [192, 160], P('gx', 'gy'), may hold values from 0 to 1, as said below
- ice_mask: int32 [192, 160], P('gx', 'gy'), may hold values from 0 to 1, as said below
- group_speed: float32 [30], replicated, may hold values from 0.1 to 0.4
- growth_rate: float32 [30], replicated, may hold values from 0.1 to 1
- dissipation: float32 [30], replicated, may hold values from 0.3 to 3
Outputs:
- adjoint_spectrum: float32 [192, 160, 1080], P('gx', 'gy')
The draws below stay inside these ranges and needn't reach their ends.
Inputs may be any that keep to these rules, and one draw needn't show every extreme that they name: `land_mask`: 1 marks land, 0 sea. `ice_mask`: 1 marks sea ice, 0 open water.
All inputs are finite; a program needn't handle non-finite values.
Results may differ from the reference program's by a relative error of at most 0.0001.
Values sent between devices are 32-bit elements; how exact they have to be, the bound alone decides.
A program may use at most 128 MiB of HBM per device.

```python
import math
import jax
import jax.numpy as jnp
from jax import lax

DIRS = 36
FREQS = 30
BINS = 1080
CX = 24
CY = 40
NX = 192
NY = 160


def draw_land_mask(key, part):
    islands = max(2, NX * NY // (8 * CX * CY))
    centre_x = jax.random.randint(jax.random.fold_in(key, 1), (islands,), 0, NX)
    centre_y = jax.random.randint(jax.random.fold_in(key, 2), (islands,), 0, NY)
    radius = jax.random.randint(jax.random.fold_in(key, 3), (islands,), max(1, min(CX, CY) // 2), max(CX, CY) + 1)
    row_index = jnp.arange(NX, dtype=jnp.int32)
    col_index = jnp.arange(NY, dtype=jnp.int32)
    gap_x = jnp.abs(row_index[None, :] - centre_x[:, None])
    gap_x = jnp.minimum(gap_x, NX - gap_x)
    gap_y = jnp.abs(col_index[None, :] - centre_y[:, None])
    inside = gap_x[:, :, None] * gap_x[:, :, None] + gap_y[:, None, :] * gap_y[:, None, :] < (radius * radius)[:, None, None]
    return jnp.any(inside, axis=0).astype(jnp.int32)


def draw_ice_mask(key, part):
    ice_reach = max(2, NY // 8)
    south_edge = jax.random.randint(jax.random.fold_in(key, 11), (NX, 1), 0, ice_reach)
    north_edge = jax.random.randint(jax.random.fold_in(key, 12), (NX, 1), 0, ice_reach)
    col_index = jnp.arange(NY, dtype=jnp.int32)[None, :]
    frozen = (col_index < south_edge) | (col_index >= NY - north_edge)
    return frozen.astype(jnp.int32)


def shard_levels(own_key, extent, split, smallest, largest):
    gain = 1.0
    for axis_at, blocks in split:
        heights = jax.random.uniform(jax.random.fold_in(jax.random.fold_in(own_key, 6), axis_at), (blocks,), jnp.float32, smallest / len(split), largest / len(split))
        gain = gain * jnp.repeat(jnp.exp(heights), extent[axis_at] // blocks).reshape((-1,) + (1,) * (len(extent) - 1 - axis_at))
    return gain


def bell_draw(own_key, shape, scale, most, split=(), held_as=jnp.bfloat16):
    loudness = shard_levels(own_key, shape, split, -0.22, 0.18) if split else 1.0
    entries = jax.random.normal(own_key, shape, jnp.float32) * scale * loudness
    return jnp.minimum(jnp.maximum(entries, -most), most).astype(held_as)


def setup_inputs(seed: int = 0) -> dict:
    key_of = jax.random.split(jax.random.key(seed), 12)
    return {
        "spectrum": jnp.clip(jnp.exp(math.log(1.0) - 2.9957323 * jax.random.uniform(key_of[0], (NX, NY, BINS), jnp.float32) ** shard_levels(key_of[0], (NX, NY, BINS), ((0, 8), (1, 4)), -0.2, 0.2)), 0.05, 1.0),
        "adjoint_in": jnp.clip(2.0 * jax.random.uniform(key_of[1], (NX, NY, BINS), jnp.float32) ** shard_levels(key_of[1], (NX, NY, BINS), ((0, 8), (1, 4)), -0.2, 0.2), 0.0, 2.0),
        "current_x": jnp.clip(jax.random.uniform(key_of[2], (NX, NY), jnp.float32, -0.08, 0.08) * shard_levels(key_of[2], (NX, NY), ((0, 8), (1, 4)), -0.4, 0.0), -0.08, 0.08),
        "current_y": jnp.clip(jax.random.uniform(key_of[3], (NX, NY), jnp.float32, -0.08, 0.08) * shard_levels(key_of[3], (NX, NY), ((0, 8), (1, 4)), -0.4, 0.0), -0.08, 0.08),
        "wind_x": bell_draw(key_of[4], (NX, NY), 1.0, 4.0, ((0, 8), (1, 4)), jnp.float32),
        "wind_y": bell_draw(key_of[5], (NX, NY), 1.0, 4.0, ((0, 8), (1, 4)), jnp.float32),
        "land_mask": draw_land_mask(jax.random.fold_in(key_of[11], 71), 0),
        "ice_mask": draw_ice_mask(jax.random.fold_in(key_of[11], 71), 0),
        "group_speed": jnp.clip(jnp.exp(jax.random.uniform(key_of[8], (FREQS,), jnp.float32, math.log(0.1), math.log(0.4))), 0.1, 0.4),
        "growth_rate": jnp.clip(jnp.exp(jax.random.uniform(key_of[9], (FREQS,), jnp.float32, math.log(0.1), math.log(1.0))), 0.1, 1.0),
        "dissipation": jnp.clip(jnp.exp(jax.random.uniform(key_of[10], (FREQS,), jnp.float32, math.log(0.3), math.log(3.0))), 0.3, 3.0),
    }


def shift_north(values):
    return jnp.concatenate([values[:, 1:], jnp.zeros_like(values[:, :1])], axis=1)


def shift_south(values):
    return jnp.concatenate([jnp.zeros_like(values[:, :1]), values[:, :-1]], axis=1)


def reference(spectrum, adjoint_in, current_x, current_y, wind_x, wind_y, land_mask, ice_mask, group_speed, growth_rate, dissipation):
    sea_mask = (1 - land_mask).astype(jnp.float32)
    ice_free = (1 - ice_mask).astype(jnp.float32)
    angles = (2.0 * math.pi / DIRS) * (jnp.arange(DIRS, dtype=jnp.float32) + 0.5)
    open_lon = sea_mask * jnp.roll(sea_mask, -1, axis=0)
    drift_lon = 0.5 * (current_x + jnp.roll(current_x, -1, axis=0))
    open_lat = sea_mask * shift_north(sea_mask)
    drift_lat = 0.5 * (current_y + shift_north(current_y))

    def forward_block(direction):
        offset = (direction * FREQS).astype(jnp.int32)
        block_field = lax.dynamic_slice_in_dim(spectrum, offset, FREQS, 2)
        cosine = jnp.cos(angles[direction])
        sine_val = jnp.sin(angles[direction])
        lon_courant = open_lon[..., None] * (group_speed * cosine + drift_lon[..., None])
        lat_courant = open_lat[..., None] * (group_speed * sine_val + drift_lat[..., None])
        lon_plus = jnp.maximum(lon_courant, 0.0)
        lon_minus = jnp.minimum(lon_courant, 0.0)
        lat_plus = jnp.maximum(lat_courant, 0.0)
        lat_minus = jnp.minimum(lat_courant, 0.0)
        lon_flux = lon_plus * block_field + lon_minus * jnp.roll(block_field, -1, axis=0)
        lat_flux = lat_plus * block_field + lat_minus * shift_north(block_field)
        advected = block_field - (lon_flux - jnp.roll(lon_flux, 1, axis=0)) - (lat_flux - shift_south(lat_flux))
        return advected, lon_plus, lon_minus, lat_plus, lat_minus, offset, cosine, sine_val

    def add_energy(direction, running):
        advected = forward_block(direction)[0]
        return running + jnp.sum(advected, axis=2)

    energy = lax.fori_loop(0, DIRS, add_energy, jnp.zeros((NX, NY), jnp.float32)) / BINS

    def weigh_block(direction):
        advected, lon_plus, lon_minus, lat_plus, lat_minus, offset, cosine, sine_val = forward_block(direction)
        incoming = lax.dynamic_slice_in_dim(adjoint_in, offset, FREQS, 2)
        project = wind_x[..., None] * cosine + wind_y[..., None] * sine_val
        gained = 1.0 + growth_rate * jnp.maximum(project, 0.0) * ice_free[..., None]
        damped = 1.0 + dissipation * energy[..., None] * advected
        weighted = incoming * gained / (damped * damped)
        return advected, weighted, lon_plus, lon_minus, lat_plus, lat_minus, offset

    def add_coupling(direction, running):
        parts = weigh_block(direction)
        advected, weighted = parts[0], parts[1]
        return running + jnp.sum(weighted * dissipation * advected * advected, axis=2)

    coupling = lax.fori_loop(0, DIRS, add_coupling, jnp.zeros((NX, NY), jnp.float32))

    def adjoint_block(direction, output):
        advected, weighted, lon_plus, lon_minus, lat_plus, lat_minus, offset = weigh_block(direction)
        sensitivity = sea_mask[..., None] * (weighted - coupling[..., None] / BINS)
        lon_step = jnp.roll(sensitivity, -1, axis=0) - sensitivity
        lat_step = shift_north(sensitivity) - sensitivity
        result = sensitivity + lon_plus * lon_step + jnp.roll(lon_minus * lon_step, 1, axis=0)
        result = result + lat_plus * lat_step + shift_south(lat_minus * lat_step)
        return lax.dynamic_update_slice_in_dim(output, result, offset, 2)

    return lax.fori_loop(0, DIRS, adjoint_block, jnp.zeros((NX, NY, BINS), jnp.float32))
```

```python
import functools
import math

import jax
import jax.numpy as jnp
import numpy as np
from jax import lax
from jax.experimental import pallas as pl
from jax.experimental.pallas import tpu as pltpu
from jax.sharding import PartitionSpec as P

DIRS = 36
LANES = 128
ANY = pl.BlockSpec(memory_space=pl.ANY)
VMEM = pl.BlockSpec(memory_space=pltpu.VMEM)


def lane_chunks(bins):
    return [(s, min(LANES, bins - s)) for s in range(0, bins, LANES)]


def up(block, last):
    return jnp.concatenate([block[1:], last], axis=0)


def down(block, first):
    return jnp.concatenate([first, block[:-1]], axis=0)


def spread(cells, stats, table, count):
    for k in range(count):
        turned = table[k][:cells, :]

        def one(i, carry, k=k, turned=turned):
            column = pltpu.roll(turned, LANES - i, axis=1)[:, 0:1]
            stats[k, i] = jnp.broadcast_to(column, (cells, LANES))
            return carry

        lax.fori_loop(1, stats.shape[1], one, 0)
        stats[k, 0] = jnp.broadcast_to(turned[:, 0:1], (cells, LANES))


def forward_kernel(
    nx, ny,
    spectrum, adjoint, cx, cy, wx, wy, land, ice, speed, growth, diss, trig,
    sens_out, lon_out, lat_out, turned_out, table_out,
    sp, adj, sens, lat, near_f, near_i, ext, face, turned, stats, flux, work, lat_s, params,
    local_sem, out_sem, far_send, far_recv,
):
    gx, gy = lax.axis_index("gx"), lax.axis_index("gy")
    rows, cells, bins = adjoint.shape
    east, west = lax.rem(gx + 1, nx), lax.rem(gx + nx - 1, nx)
    has_north, has_south = gy < ny - 1, gy > 0
    chunks = lane_chunks(bins)
    pad = stats.shape[2]

    barrier = pltpu.get_barrier_semaphore()
    for axis, where in (("gx", east), ("gx", west)):
        pl.semaphore_signal(barrier, inc=1, device_id={axis: where}, device_id_type=pl.DeviceIdType.MESH)

    @pl.when(has_north)
    def _():
        pl.semaphore_signal(barrier, inc=1, device_id={"gy": gy + 1}, device_id_type=pl.DeviceIdType.MESH)

    @pl.when(has_south)
    def _():
        pl.semaphore_signal(barrier, inc=1, device_id={"gy": gy - 1}, device_id_type=pl.DeviceIdType.MESH)

    half = rows // 2
    loads = []
    for n, (src, dst, off) in enumerate(((spectrum, sp, 1), (adjoint, adj, 0))):
        for m in range(2):
            loads.append(
                pltpu.make_async_copy(
                    src.at[pl.ds(m * half, half)], dst.at[pl.ds(m * half + off, half)], local_sem.at[2 * n + m]
                )
            )
    for copy in loads:
        copy.start()

    def far(src, dst, n, axis, where):
        return pltpu.make_async_remote_copy(
            src_ref=src, dst_ref=dst, send_sem=far_send.at[n], recv_sem=far_recv.at[n],
            device_id={axis: where}, device_id_type=pl.DeviceIdType.MESH,
        )

    to_east = [
        far(cx, near_f.at[0], 0, "gx", east),
        far(land, near_i.at[0], 1, "gx", east),
        far(spectrum.at[rows - 1], sp.at[0], 2, "gx", east),
    ]
    to_west = [
        far(cx, near_f.at[1], 3, "gx", west),
        far(land, near_i.at[1], 4, "gx", west),
        far(spectrum.at[0], sp.at[rows + 1], 5, "gx", west),
    ]
    to_north = [
        far(cy, near_f.at[2], 6, "gy", gy + 1),
        far(land, near_i.at[2], 7, "gy", gy + 1),
        far(spectrum.at[:, pl.ds(cells - 1, 1), :], lat.at[0], 8, "gy", gy + 1),
    ]
    to_south = [
        far(cy, near_f.at[3], 9, "gy", gy - 1),
        far(land, near_i.at[3], 10, "gy", gy - 1),
        far(spectrum.at[:, pl.ds(0, 1), :], lat.at[1], 11, "gy", gy - 1),
    ]

    @pl.when(jnp.logical_not(has_south))
    def _():
        lat[0] = jnp.zeros(lat.shape[1:], jnp.float32)

    @pl.when(jnp.logical_not(has_north))
    def _():
        lat[1] = jnp.zeros(lat.shape[1:], jnp.float32)

    pl.semaphore_wait(barrier, 2 + has_north.astype(jnp.int32) + has_south.astype(jnp.int32))

    def each_lat(method, first=0, last=3):
        @pl.when(has_north)
        def _():
            for copy in to_north[first:last]:
                getattr(copy, method)()

        @pl.when(has_south)
        def _():
            for copy in to_south[first:last]:
                getattr(copy, method)()

    def lat_arrives(first, last):
        @pl.when(has_south)
        def _():
            for copy in to_north[first:last]:
                copy.wait_recv()

        @pl.when(has_north)
        def _():
            for copy in to_south[first:last]:
                copy.wait_recv()

    each_lat("start", 2, 3)
    for copy in to_east[2:] + to_west[2:]:
        copy.start()
    for copy in to_east[:2] + to_west[:2]:
        copy.start()
    each_lat("start", 0, 2)

    freqs = speed.shape[1]
    params[...] = jnp.zeros(params.shape, jnp.float32)
    params[0:1, 0:freqs] = speed[...]
    params[1:2, 0:freqs] = growth[...]
    params[2:3, 0:freqs] = diss[...]
    spots = lax.rem(lax.broadcasted_iota(jnp.int32, (params.shape[1], bins), 1), freqs)
    hot = (spots == lax.broadcasted_iota(jnp.int32, (params.shape[1], bins), 0)).astype(jnp.float32)
    by_bin = jnp.dot(params[...], hot, precision=lax.Precision.HIGHEST, preferred_element_type=jnp.float32)
    cosine, sine = trig[0:1], trig[1:2]
    table_out[0:1] = by_bin[0:1] * cosine
    table_out[1:2] = by_bin[0:1] * sine
    table_out[2:3] = by_bin[1:2] * cosine
    table_out[3:4] = by_bin[1:2] * sine
    table_out[4:5] = by_bin[2:3]
    table = table_out

    for copy in to_east[:2] + to_west[:2]:
        copy.wait_recv()
    lat_arrives(0, 2)
    ext[...] = jnp.zeros(ext.shape, jnp.float32)
    sea_of = lambda mask: (1 - mask).astype(jnp.float32)
    ext[0, 0:1, 0:cells] = near_f[0, rows - 1 : rows]
    ext[0, 1 : rows + 1, 0:cells] = cx[...]
    ext[0, rows + 1 : rows + 2, 0:cells] = near_f[1, 0:1]
    ext[1, 0:1, 0:cells] = sea_of(near_i[0, rows - 1 : rows])
    ext[1, 1 : rows + 1, 0:cells] = sea_of(land[...])
    ext[1, rows + 1 : rows + 2, 0:cells] = sea_of(near_i[1, 0:1])
    ext[2, 0:rows, 0:cells] = cy[...]
    ext[3, 0:rows, 0:cells] = sea_of(land[...])
    ext[4, 0:rows, 0:cells] = near_f[2]
    ext[5, 0:rows, 0:cells] = sea_of(near_i[2])
    ext[6, 0:rows, 0:cells] = near_f[3]
    ext[7, 0:rows, 0:cells] = sea_of(near_i[3])
    face[...] = jnp.zeros(face.shape, jnp.float32)
    opened = ext[1, 0 : rows + 1] * ext[1, 1 : rows + 2]
    face[0, 0 : rows + 1] = opened
    face[1, 0 : rows + 1] = opened * (0.5 * (ext[0, 0 : rows + 1] + ext[0, 1 : rows + 2]))
    tall = ext.shape[1]
    lane = lax.broadcasted_iota(jnp.int32, (tall, LANES), 1)

    def pair(own, south, north):
        mine = jnp.where(lane == cells, pltpu.roll(own, cells, axis=1), own)
        other = jnp.where(lane == cells - 1, pltpu.roll(north, cells - 1, axis=1), pltpu.roll(own, LANES - 1, axis=1))
        other = jnp.where(lane == cells, pltpu.roll(south, 1, axis=1), other)
        return mine, other

    sea_a, sea_b = pair(ext[3], ext[5], ext[7])
    cy_a, cy_b = pair(ext[2], ext[4], ext[6])
    closed = jnp.logical_or(
        jnp.logical_and(lane == cells, jnp.logical_not(has_south)),
        jnp.logical_and(lane == cells - 1, jnp.logical_not(has_north)),
    )
    opened = sea_a * sea_b
    face[2, 0:tall] = jnp.where(closed, 0.0, opened)
    face[3, 0:tall] = jnp.where(closed, 0.0, opened * (0.5 * (cy_a + cy_b)))
    ice_free = sea_of(ice[...])
    face[4, 0:rows, 0:cells] = wx[...] * ice_free
    face[5, 0:rows, 0:cells] = wy[...] * ice_free
    face[6, 0:rows, 0:cells] = sea_of(land[...])
    for k in range(7):
        turned[k] = face[k].T
    turned_out[...] = turned[0:4, 0:pad]
    spread(pad, stats, turned, 7)

    for copy in loads:
        copy.wait()
    for copy in to_east[2:] + to_west[2:]:
        copy.wait_recv()
    lat_arrives(2, 3)

    def lon_flux(f, s, w):
        courant = stats[0, f, 0:cells, 0:w] * table[0:1, s : s + w] + stats[1, f, 0:cells, 0:w]
        return courant * jnp.where(courant > 0, sp[f, :, s : s + w], sp[f + 1, :, s : s + w])

    lon_send = [
        far(sens.at[rows - 1], lon_out.at[0], 12, "gx", east),
        far(sens.at[0], lon_out.at[1], 13, "gx", west),
    ]
    lat_north = [far(lat_s.at[1, pl.ds(m * half, half)], lat_out.at[0, pl.ds(m * half, half)], 14 + m, "gy", gy + 1) for m in range(2)]
    lat_south = [far(lat_s.at[0, pl.ds(m * half, half)], lat_out.at[1, pl.ds(m * half, half)], 16 + m, "gy", gy - 1) for m in range(2)]

    def lat_send(m):
        @pl.when(has_north)
        def _():
            lat_north[m].start()

        @pl.when(has_south)
        def _():
            lat_south[m].start()

    def send_row(i):
        return pltpu.make_async_copy(sens.at[i], sens_out.at[i], out_sem.at[i])

    def row(k, carry):
        i = lax.rem(k + rows - 1, rows)

        @pl.when(k < 2)
        def _():
            for s, w in chunks:
                flux[:, s : s + w] = lon_flux(i, s, w)

        @pl.when(k == 2)
        def _():
            for copy in lon_send:
                copy.start()

        @pl.when(k == half + 2)
        def _():
            lat_send(0)

        energy = jnp.zeros((cells, 1), jnp.float32)
        total = jnp.zeros((cells, LANES), jnp.float32)
        for s, w in chunks:
            own = sp[i + 1, :, s : s + w]
            fx = lon_flux(i + 1, s, w)
            fx_low = flux[:, s : s + w]
            sin_row = table[1:2, s : s + w]
            courant = stats[2, i, 0:cells, 0:w] * sin_row + stats[3, i, 0:cells, 0:w]
            fy = courant * jnp.where(courant > 0, own, up(own, lat[1, i, :, s : s + w]))
            low = stats[2, i, cells : cells + 1, 0:w] * sin_row + stats[3, i, cells : cells + 1, 0:w]
            fy_low = down(fy, low * jnp.where(low > 0, lat[0, i, :, s : s + w], own[0:1]))
            advected = own - (fx - fx_low) - (fy - fy_low)
            flux[:, s : s + w] = fx
            work[:, s : s + w] = advected
            if w == LANES:
                total = total + advected
            else:
                energy = energy + jnp.sum(advected, axis=1, keepdims=True)
        energy = (energy + jnp.sum(total, axis=1, keepdims=True)) * (1.0 / bins)
        energy = jnp.broadcast_to(energy, (cells, LANES))
        coupling = jnp.zeros((cells, 1), jnp.float32)
        total = jnp.zeros((cells, LANES), jnp.float32)
        for s, w in chunks:
            advected = work[:, s : s + w]
            blow = stats[4, i, 0:cells, 0:w] * table[2:3, s : s + w] + stats[5, i, 0:cells, 0:w] * table[3:4, s : s + w]
            gain = 1.0 + jnp.maximum(blow, 0.0)
            scaled = table[4:5, s : s + w] * advected
            damp = 1.0 + energy[:, 0:w] * scaled
            weighted = adj[i, :, s : s + w] * gain / (damp * damp)
            sens[i, :, s : s + w] = weighted
            term = weighted * scaled * advected
            if w == LANES:
                total = total + term
            else:
                coupling = coupling + jnp.sum(term, axis=1, keepdims=True)
        coupling = (coupling + jnp.sum(total, axis=1, keepdims=True)) * (1.0 / bins)
        coupling = jnp.broadcast_to(coupling, (cells, LANES))
        for s, w in chunks:
            value = stats[6, i, 0:cells, 0:w] * (sens[i, :, s : s + w] - coupling[:, 0:w])
            sens[i, :, s : s + w] = value
            lat_s[0, i, :, s : s + w] = value[0:1]
            lat_s[1, i, :, s : s + w] = value[cells - 1 : cells]

        @pl.when(k > 0)
        def _():
            send_row(lax.rem(k + rows - 2, rows)).start()

        return carry

    lax.fori_loop(0, rows, row, 0)
    lat_send(1)
    send_row(rows - 2).start()

    fill = [pltpu.make_async_copy(lat.at[m], lat_out.at[m], local_sem.at[m]) for m in range(2)]
    for m, there in ((0, has_south), (1, has_north)):
        @pl.when(jnp.logical_not(there))
        def _(m=m):
            fill[m].start()

    for copy in to_east + to_west:
        copy.wait_send()
    each_lat("wait_send")
    for copy in lon_send:
        copy.wait()

    @pl.when(has_north)
    def _():
        for copy in lat_north:
            copy.wait_send()
        for copy in lat_south:
            copy.wait_recv()

    @pl.when(has_south)
    def _():
        for copy in lat_south:
            copy.wait_send()
        for copy in lat_north:
            copy.wait_recv()

    for m, there in ((0, has_south), (1, has_north)):
        @pl.when(jnp.logical_not(there))
        def _(m=m):
            fill[m].wait()

    def finish(i, carry):
        send_row(i).wait()
        return carry

    lax.fori_loop(0, rows, finish, 0)


def transpose_kernel(
    sens, lon, lat, turned, table, out,
    ext, stats, held, done, in_sem, out_sem,
):
    rows, cells, bins = sens.shape
    chunks = lane_chunks(bins)
    pad = stats.shape[2]
    groups = in_sem.shape[0] - 2
    size = rows // groups
    edges = [pltpu.make_async_copy(lon.at[m], ext.at[m * (rows + 1)], in_sem.at[groups + m]) for m in range(2)]
    part = lambda g: pltpu.make_async_copy(sens.at[pl.ds(g * size, size)], ext.at[pl.ds(g * size + 1, size)], in_sem.at[g])
    edges[0].start()
    for g in range(groups):
        part(g).start()
    edges[1].start()
    spread(pad, stats, turned, 4)
    edges[0].wait()
    part(0).wait()

    def lon_face(f, s, w):
        return stats[0, f, 0:cells, 0:w] * table[0:1, s : s + w] + stats[1, f, 0:cells, 0:w]

    for s, w in chunks:
        held[:, s : s + w] = jnp.minimum(lon_face(0, s, w), 0.0) * (ext[1, :, s : s + w] - ext[0, :, s : s + w])

    send = lambda i: pltpu.make_async_copy(done.at[i], out.at[i], out_sem.at[i])

    def row(i, carry):
        @pl.when(jnp.logical_and(lax.rem(i, size) == size - 1, i < rows - 1))
        def _():
            part(i // size + 1).wait()

        @pl.when(i == rows - 1)
        def _():
            edges[1].wait()

        for s, w in chunks:
            own = ext[i + 1, :, s : s + w]
            step = ext[i + 2, :, s : s + w] - own
            courant = lon_face(i + 1, s, w)
            value = own + held[:, s : s + w] + jnp.maximum(courant, 0.0) * step
            held[:, s : s + w] = jnp.minimum(courant, 0.0) * step
            sin_row = table[1:2, s : s + w]
            courant = stats[2, i, 0:cells, 0:w] * sin_row + stats[3, i, 0:cells, 0:w]
            step = up(own, lat[1, i, :, s : s + w]) - own
            value = value + jnp.maximum(courant, 0.0) * step
            low = stats[2, i, cells : cells + 1, 0:w] * sin_row + stats[3, i, cells : cells + 1, 0:w]
            low = jnp.minimum(low, 0.0) * (own[0:1] - lat[0, i, :, s : s + w])
            done[i, :, s : s + w] = value + down(jnp.minimum(courant, 0.0) * step, low)

        @pl.when(i > 0)
        def _():
            send(i - 1).start()

        return carry

    lax.fori_loop(0, rows, row, 0)
    send(rows - 1).start()

    def finish(i, carry):
        send(i).wait()
        return carry

    lax.fori_loop(0, rows, finish, 0)


def round_up(value, step):
    return (value + step - 1) // step * step


def body(nx, ny, spectrum, adjoint_in, cx, cy, wx, wy, land, ice, speed, growth, diss):
    rows, cells, bins = spectrum.shape
    freqs = speed.shape[0]
    angles = 2.0 * math.pi / DIRS * (np.arange(DIRS) + 0.5)
    trig = np.stack([np.repeat(np.cos(angles), freqs), np.repeat(np.sin(angles), freqs)]).astype(np.float32)
    pad = round_up(cells + 1, 8)
    tall = round_up(rows + 2, 8)
    f32 = jnp.float32
    dma = pltpu.SemaphoreType.DMA
    shape = jax.ShapeDtypeStruct
    sens, lon, lat, turned, table = pl.pallas_call(
        functools.partial(forward_kernel, nx, ny),
        out_shape=(
            shape((rows, cells, bins), f32),
            shape((2, cells, bins), f32),
            shape((2, rows, 1, bins), f32),
            shape((4, pad, LANES), f32),
            shape((8, bins), f32),
        ),
        in_specs=[ANY, ANY] + [VMEM] * 10,
        out_specs=(ANY, ANY, ANY, VMEM, VMEM),
        scratch_shapes=[
            pltpu.VMEM((rows + 2, cells, bins), f32),
            pltpu.VMEM((rows, cells, bins), f32),
            pltpu.VMEM((rows, cells, bins), f32),
            pltpu.VMEM((2, rows, 1, bins), f32),
            pltpu.VMEM((4, rows, cells), f32),
            pltpu.VMEM((4, rows, cells), jnp.int32),
            pltpu.VMEM((8, tall, LANES), f32),
            pltpu.VMEM((7, LANES, LANES), f32),
            pltpu.VMEM((7, LANES, LANES), f32),
            pltpu.VMEM((7, rows + 1, pad, LANES), f32),
            pltpu.VMEM((cells, bins), f32),
            pltpu.VMEM((cells, bins), f32),
            pltpu.VMEM((2, rows, 1, bins), f32),
            pltpu.VMEM((8, round_up(freqs, 8)), f32),
            dma((4,)),
            dma((rows,)),
            dma((18,)),
            dma((18,)),
        ],
        compiler_params=pltpu.CompilerParams(
            collective_id=0, has_side_effects=True, vmem_limit_bytes=40 * 2**20
        ),
        name="forward",
    )(spectrum, adjoint_in, cx, cy, wx, wy, land, ice,
      speed.reshape(1, -1), growth.reshape(1, -1), diss.reshape(1, -1), jnp.asarray(trig))
    groups = max(g for g in (1, 2, 3, 4, 6) if rows % g == 0)
    return pl.pallas_call(
        transpose_kernel,
        out_shape=shape((rows, cells, bins), f32),
        in_specs=[ANY, ANY, VMEM, VMEM, VMEM],
        out_specs=ANY,
        scratch_shapes=[
            pltpu.VMEM((rows + 2, cells, bins), f32),
            pltpu.VMEM((4, rows + 1, pad, LANES), f32),
            pltpu.VMEM((cells, bins), f32),
            pltpu.VMEM((rows, cells, bins), f32),
            dma((groups + 2,)),
            dma((rows,)),
        ],
        compiler_params=pltpu.CompilerParams(vmem_limit_bytes=32 * 2**20),
        name="transpose",
    )(sens, lon, lat, turned, table)


def solution(mesh):
    grid = P("gx", "gy")
    field = P("gx", "gy", None)
    return jax.shard_map(
        functools.partial(body, mesh.shape["gx"], mesh.shape["gy"]),
        mesh=mesh,
        in_specs=(field, field) + (grid,) * 6 + (P(), P(), P()),
        out_specs=field,
        check_vma=False,
    )
```

```python
import functools
import math

import jax
import jax.numpy as jnp
import numpy as np
from jax import lax
from jax.experimental import pallas as pl
from jax.experimental.pallas import tpu as pltpu
from jax.sharding import PartitionSpec as P

DIRS = 36
LANES = 128
HBM = pl.BlockSpec(memory_space=pltpu.HBM)
VMEM = pl.BlockSpec(memory_space=pltpu.VMEM)


def lane_chunks(bins):
    return [(s, min(LANES, bins - s)) for s in range(0, bins, LANES)]


def up(block, last):
    return jnp.concatenate([block[1:], last], axis=0)


def down(block, first):
    return jnp.concatenate([first, block[:-1]], axis=0)


def spread(cells, stats, table, count):
    for k in range(count):
        turned = table[k][:cells, :]

        def one(i, carry, k=k, turned=turned):
            column = pltpu.roll(turned, LANES - i, axis=1)[:, 0:1]
            stats[k, i] = jnp.broadcast_to(column, (cells, LANES))
            return carry

        lax.fori_loop(1, stats.shape[1], one, 0, unroll=4)
        stats[k, 0] = jnp.broadcast_to(turned[:, 0:1], (cells, LANES))


def forward_kernel(
    nx, ny,
    spectrum, adjoint, cx_h, cy_h, wx_h, wy_h, land_h, ice_h, speed_h, growth_h, diss_h, trig_h,
    sens, lat_out, stats, table,
    sp, adj, lat, rim, near_f, near_i, mine_f, mine_i, coeffs, trig, ext, face, turned, flux, work, lat_s, params,
    local_sem, far_send, far_recv,
):
    gx, gy = lax.axis_index("gx"), lax.axis_index("gy")
    rows, cells, bins = adjoint.shape
    east, west = lax.rem(gx + 1, nx), lax.rem(gx + nx - 1, nx)
    has_north, has_south = gy < ny - 1, gy > 0
    chunks = lane_chunks(bins)
    pad = stats.shape[2]

    barrier = pltpu.get_barrier_semaphore()
    for axis, where in (("gx", east), ("gx", west)):
        pl.semaphore_signal(barrier, inc=1, device_id={axis: where}, device_id_type=pl.DeviceIdType.MESH)

    @pl.when(has_north)
    def _():
        pl.semaphore_signal(barrier, inc=1, device_id={"gy": gy + 1}, device_id_type=pl.DeviceIdType.MESH)

    @pl.when(has_south)
    def _():
        pl.semaphore_signal(barrier, inc=1, device_id={"gy": gy - 1}, device_id_type=pl.DeviceIdType.MESH)

    half = rows // 2
    small = []
    cx, cy, wx, wy = (mine_f.at[m] for m in range(4))
    land, ice = (mine_i.at[m] for m in range(2))
    speed, growth, diss = (coeffs.at[m] for m in range(3))
    pairs = (
        (spectrum.at[:, pl.ds(0, 1), :], rim.at[0]), (spectrum.at[:, pl.ds(cells - 1, 1), :], rim.at[1]),
        (cx_h, cx), (cy_h, cy), (land_h, land), (ice_h, ice), (wx_h, wx), (wy_h, wy),
        (speed_h, speed), (growth_h, growth), (diss_h, diss), (trig_h, trig),
    )
    for m, (src, dst) in enumerate(pairs):
        small.append(pltpu.make_async_copy(src, dst, local_sem.at[4 + m]))
    for copy in small:
        copy.start()
    loads = []
    for n, (src, dst, off) in enumerate(((spectrum, sp, 1), (adjoint, adj, 0))):
        for m in range(2):
            loads.append(
                pltpu.make_async_copy(
                    src.at[pl.ds(m * half, half)], dst.at[pl.ds(m * half + off, half)], local_sem.at[2 * n + m]
                )
            )
    for copy in loads:
        copy.start()

    def far(src, dst, n, axis, where):
        return pltpu.make_async_remote_copy(
            src_ref=src, dst_ref=dst, send_sem=far_send.at[n], recv_sem=far_recv.at[n],
            device_id={axis: where}, device_id_type=pl.DeviceIdType.MESH,
        )

    to_east = [
        far(cx_h, near_f.at[0], 0, "gx", east),
        far(land_h, near_i.at[0], 1, "gx", east),
        far(spectrum.at[rows - 1], sp.at[0], 2, "gx", east),
    ]
    to_west = [
        far(cx_h, near_f.at[1], 3, "gx", west),
        far(land_h, near_i.at[1], 4, "gx", west),
        far(spectrum.at[0], sp.at[rows + 1], 5, "gx", west),
    ]
    to_north = [
        far(cy_h, near_f.at[2], 6, "gy", gy + 1),
        far(land_h, near_i.at[2], 7, "gy", gy + 1),
        far(rim.at[1], lat.at[0], 8, "gy", gy + 1),
    ]
    to_south = [
        far(cy_h, near_f.at[3], 9, "gy", gy - 1),
        far(land_h, near_i.at[3], 10, "gy", gy - 1),
        far(rim.at[0], lat.at[1], 11, "gy", gy - 1),
    ]

    @pl.when(jnp.logical_not(has_south))
    def _():
        lat[0] = jnp.zeros(lat.shape[1:], jnp.float32)

    @pl.when(jnp.logical_not(has_north))
    def _():
        lat[1] = jnp.zeros(lat.shape[1:], jnp.float32)

    pl.semaphore_wait(barrier, 2 + has_north.astype(jnp.int32) + has_south.astype(jnp.int32))

    def each_lat(method, first=0, last=3):
        @pl.when(has_north)
        def _():
            for copy in to_north[first:last]:
                getattr(copy, method)()

        @pl.when(has_south)
        def _():
            for copy in to_south[first:last]:
                getattr(copy, method)()

    def lat_arrives(first, last):
        @pl.when(has_south)
        def _():
            for copy in to_north[first:last]:
                copy.wait_recv()

        @pl.when(has_north)
        def _():
            for copy in to_south[first:last]:
                copy.wait_recv()

    for copy in to_east[:2] + to_west[:2]:
        copy.start()
    each_lat("start", 0, 2)
    small[0].wait()
    small[1].wait()
    each_lat("start", 2, 3)
    for copy in to_east[2:] + to_west[2:]:
        copy.start()
    for copy in small[2:]:
        copy.wait()

    freqs = coeffs.shape[2]
    params[...] = jnp.zeros(params.shape, jnp.float32)
    params[0:1, 0:freqs] = speed[...]
    params[1:2, 0:freqs] = growth[...]
    params[2:3, 0:freqs] = diss[...]
    spots = lax.rem(lax.broadcasted_iota(jnp.int32, (params.shape[1], bins), 1), freqs)
    hot = (spots == lax.broadcasted_iota(jnp.int32, (params.shape[1], bins), 0)).astype(jnp.float32)
    by_bin = jnp.dot(params[...], hot, precision=lax.Precision.HIGHEST, preferred_element_type=jnp.float32)
    cosine, sine = trig[0:1], trig[1:2]
    table[0:1] = by_bin[0:1] * cosine
    table[1:2] = by_bin[0:1] * sine
    table[2:3] = by_bin[1:2] * cosine
    table[3:4] = by_bin[1:2] * sine
    table[4:5] = by_bin[2:3]

    for copy in to_east[:2] + to_west[:2]:
        copy.wait_recv()
    lat_arrives(0, 2)
    ext[...] = jnp.zeros(ext.shape, jnp.float32)
    sea_of = lambda mask: (1 - mask).astype(jnp.float32)
    ext[0, 0:1, 0:cells] = near_f[0, rows - 1 : rows]
    ext[0, 1 : rows + 1, 0:cells] = cx[...]
    ext[0, rows + 1 : rows + 2, 0:cells] = near_f[1, 0:1]
    ext[1, 0:1, 0:cells] = sea_of(near_i[0, rows - 1 : rows])
    ext[1, 1 : rows + 1, 0:cells] = sea_of(land[...])
    ext[1, rows + 1 : rows + 2, 0:cells] = sea_of(near_i[1, 0:1])
    ext[2, 0:rows, 0:cells] = cy[...]
    ext[3, 0:rows, 0:cells] = sea_of(land[...])
    ext[4, 0:rows, 0:cells] = near_f[2]
    ext[5, 0:rows, 0:cells] = sea_of(near_i[2])
    ext[6, 0:rows, 0:cells] = near_f[3]
    ext[7, 0:rows, 0:cells] = sea_of(near_i[3])
    face[...] = jnp.zeros(face.shape, jnp.float32)
    opened = ext[1, 0 : rows + 1] * ext[1, 1 : rows + 2]
    face[0, 0 : rows + 1] = opened
    face[1, 0 : rows + 1] = opened * (0.5 * (ext[0, 0 : rows + 1] + ext[0, 1 : rows + 2]))
    tall = ext.shape[1]
    lane = lax.broadcasted_iota(jnp.int32, (tall, LANES), 1)

    def pair(own, south, north):
        mine = jnp.where(lane == cells, pltpu.roll(own, cells, axis=1), own)
        other = jnp.where(lane == cells - 1, pltpu.roll(north, cells - 1, axis=1), pltpu.roll(own, LANES - 1, axis=1))
        other = jnp.where(lane == cells, pltpu.roll(south, 1, axis=1), other)
        return mine, other

    sea_a, sea_b = pair(ext[3], ext[5], ext[7])
    cy_a, cy_b = pair(ext[2], ext[4], ext[6])
    closed = jnp.logical_or(
        jnp.logical_and(lane == cells, jnp.logical_not(has_south)),
        jnp.logical_and(lane == cells - 1, jnp.logical_not(has_north)),
    )
    opened = sea_a * sea_b
    face[2, 0:tall] = jnp.where(closed, 0.0, opened)
    face[3, 0:tall] = jnp.where(closed, 0.0, opened * (0.5 * (cy_a + cy_b)))
    ice_free = sea_of(ice[...])
    face[4, 0:rows, 0:cells] = wx[...] * ice_free
    face[5, 0:rows, 0:cells] = wy[...] * ice_free
    face[6, 0:rows, 0:cells] = sea_of(land[...])
    for k in range(7):
        turned[k] = face[k].T
    spread(pad, stats, turned, 7)

    for copy in loads:
        copy.wait()
    for copy in to_east[2:] + to_west[2:]:
        copy.wait_recv()
    lat_arrives(2, 3)

    def lon_flux(f, s, w):
        courant = stats[0, f, 0:cells, 0:w] * table[0:1, s : s + w] + stats[1, f, 0:cells, 0:w]
        return courant * jnp.where(courant > 0, sp[f, :, s : s + w], sp[f + 1, :, s : s + w])

    lon_send = [
        far(sens.at[rows], sens.at[0], 12, "gx", east),
        far(sens.at[1], sens.at[rows + 1], 13, "gx", west),
    ]
    lat_north = [far(lat_s.at[1, pl.ds(m * half, half)], lat_out.at[0, pl.ds(m * half, half)], 14 + m, "gy", gy + 1) for m in range(2)]
    lat_south = [far(lat_s.at[0, pl.ds(m * half, half)], lat_out.at[1, pl.ds(m * half, half)], 16 + m, "gy", gy - 1) for m in range(2)]

    def lat_send(m):
        @pl.when(has_north)
        def _():
            lat_north[m].start()

        @pl.when(has_south)
        def _():
            lat_south[m].start()

    def row(k, carry):
        i = lax.rem(k + rows - 1, rows)

        @pl.when(k < 2)
        def _():
            for s, w in chunks:
                flux[:, s : s + w] = lon_flux(i, s, w)

        @pl.when(k == 2)
        def _():
            for copy in lon_send:
                copy.start()

        @pl.when(k == half + 2)
        def _():
            lat_send(0)

        energy = jnp.zeros((cells, 1), jnp.float32)
        total = jnp.zeros((cells, LANES), jnp.float32)
        for s, w in chunks:
            own = sp[i + 1, :, s : s + w]
            fx = lon_flux(i + 1, s, w)
            fx_low = flux[:, s : s + w]
            sin_row = table[1:2, s : s + w]
            courant = stats[2, i, 0:cells, 0:w] * sin_row + stats[3, i, 0:cells, 0:w]
            fy = courant * jnp.where(courant > 0, own, up(own, lat[1, i, :, s : s + w]))
            low = stats[2, i, cells : cells + 1, 0:w] * sin_row + stats[3, i, cells : cells + 1, 0:w]
            fy_low = down(fy, low * jnp.where(low > 0, lat[0, i, :, s : s + w], own[0:1]))
            advected = own - (fx - fx_low) - (fy - fy_low)
            flux[:, s : s + w] = fx
            work[:, s : s + w] = advected
            if w == LANES:
                total = total + advected
            else:
                energy = energy + jnp.sum(advected, axis=1, keepdims=True)
        energy = (energy + jnp.sum(total, axis=1, keepdims=True)) * (1.0 / bins)
        energy = jnp.broadcast_to(energy, (cells, LANES))
        coupling = jnp.zeros((cells, 1), jnp.float32)
        total = jnp.zeros((cells, LANES), jnp.float32)
        for s, w in chunks:
            advected = work[:, s : s + w]
            blow = stats[4, i, 0:cells, 0:w] * table[2:3, s : s + w] + stats[5, i, 0:cells, 0:w] * table[3:4, s : s + w]
            gain = 1.0 + jnp.maximum(blow, 0.0)
            scaled = table[4:5, s : s + w] * advected
            damp = 1.0 + energy[:, 0:w] * scaled
            weighted = adj[i, :, s : s + w] * gain / (damp * damp)
            sens[i + 1, :, s : s + w] = weighted
            term = weighted * scaled * advected
            if w == LANES:
                total = total + term
            else:
                coupling = coupling + jnp.sum(term, axis=1, keepdims=True)
        coupling = (coupling + jnp.sum(total, axis=1, keepdims=True)) * (1.0 / bins)
        coupling = jnp.broadcast_to(coupling, (cells, LANES))
        for s, w in chunks:
            value = stats[6, i, 0:cells, 0:w] * (sens[i + 1, :, s : s + w] - coupling[:, 0:w])
            sens[i + 1, :, s : s + w] = value
            lat_s[0, i, :, s : s + w] = value[0:1]
            lat_s[1, i, :, s : s + w] = value[cells - 1 : cells]

        return carry

    lax.fori_loop(0, rows, row, 0)
    lat_send(1)

    fill = [pltpu.make_async_copy(lat.at[m], lat_out.at[m], local_sem.at[m]) for m in range(2)]
    for m, there in ((0, has_south), (1, has_north)):
        @pl.when(jnp.logical_not(there))
        def _(m=m):
            fill[m].start()

    for copy in to_east + to_west:
        copy.wait_send()
    each_lat("wait_send")
    for copy in lon_send:
        copy.wait()

    @pl.when(has_north)
    def _():
        for copy in lat_north:
            copy.wait_send()
        for copy in lat_south:
            copy.wait_recv()

    @pl.when(has_south)
    def _():
        for copy in lat_south:
            copy.wait_send()
        for copy in lat_north:
            copy.wait_recv()

    for m, there in ((0, has_south), (1, has_north)):
        @pl.when(jnp.logical_not(there))
        def _(m=m):
            fill[m].wait()


def transpose_kernel(ext, lat, stats, table, out, held, done, out_sem):
    rows, cells, bins = out.shape
    chunks = lane_chunks(bins)

    def lon_face(f, s, w):
        return stats[0, f, 0:cells, 0:w] * table[0:1, s : s + w] + stats[1, f, 0:cells, 0:w]

    for s, w in chunks:
        held[:, s : s + w] = jnp.minimum(lon_face(0, s, w), 0.0) * (ext[1, :, s : s + w] - ext[0, :, s : s + w])

    send = lambda i: pltpu.make_async_copy(done.at[i], out.at[i], out_sem.at[i])

    def row(i, carry):
        for s, w in chunks:
            own = ext[i + 1, :, s : s + w]
            step = ext[i + 2, :, s : s + w] - own
            courant = lon_face(i + 1, s, w)
            value = own + held[:, s : s + w] + jnp.maximum(courant, 0.0) * step
            held[:, s : s + w] = jnp.minimum(courant, 0.0) * step
            sin_row = table[1:2, s : s + w]
            courant = stats[2, i, 0:cells, 0:w] * sin_row + stats[3, i, 0:cells, 0:w]
            step = up(own, lat[1, i, :, s : s + w]) - own
            value = value + jnp.maximum(courant, 0.0) * step
            low = stats[2, i, cells : cells + 1, 0:w] * sin_row + stats[3, i, cells : cells + 1, 0:w]
            low = jnp.minimum(low, 0.0) * (own[0:1] - lat[0, i, :, s : s + w])
            done[i, :, s : s + w] = value + down(jnp.minimum(courant, 0.0) * step, low)

        @pl.when(i > 0)
        def _():
            send(i - 1).start()

        return carry

    lax.fori_loop(0, rows, row, 0)
    send(rows - 1).start()

    def finish(i, carry):
        send(i).wait()
        return carry

    lax.fori_loop(0, rows, finish, 0)


def keep(array):
    return pltpu.with_memory_space_constraint(array, pltpu.HBM)


def round_up(value, step):
    return (value + step - 1) // step * step


def body(nx, ny, spectrum, adjoint_in, cx, cy, wx, wy, land, ice, speed, growth, diss):
    rows, cells, bins = spectrum.shape
    freqs = speed.shape[0]
    angles = 2.0 * math.pi / DIRS * (np.arange(DIRS) + 0.5)
    trig = np.stack([np.repeat(np.cos(angles), freqs), np.repeat(np.sin(angles), freqs)]).astype(np.float32)
    pad = round_up(cells + 1, 8)
    tall = round_up(rows + 2, 8)
    f32 = jnp.float32
    dma = pltpu.SemaphoreType.DMA
    shape = jax.ShapeDtypeStruct
    sens, lat, stats, table = pl.pallas_call(
        functools.partial(forward_kernel, nx, ny),
        out_shape=(
            shape((rows + 2, cells, bins), f32),
            shape((2, rows, 1, bins), f32),
            shape((7, rows + 1, pad, LANES), f32),
            shape((8, bins), f32),
        ),
        in_specs=[HBM] * 12,
        out_specs=(VMEM,) * 4,
        scratch_shapes=[
            pltpu.VMEM((rows + 2, cells, bins), f32),
            pltpu.VMEM((rows, cells, bins), f32),
            pltpu.VMEM((2, rows, 1, bins), f32),
            pltpu.VMEM((2, rows, 1, bins), f32),
            pltpu.VMEM((4, rows, cells), f32),
            pltpu.VMEM((4, rows, cells), jnp.int32),
            pltpu.VMEM((4, rows, cells), f32),
            pltpu.VMEM((2, rows, cells), jnp.int32),
            pltpu.VMEM((3, 1, freqs), f32),
            pltpu.VMEM((2, bins), f32),
            pltpu.VMEM((8, tall, LANES), f32),
            pltpu.VMEM((7, LANES, LANES), f32),
            pltpu.VMEM((7, LANES, LANES), f32),
            pltpu.VMEM((cells, bins), f32),
            pltpu.VMEM((cells, bins), f32),
            pltpu.VMEM((2, rows, 1, bins), f32),
            pltpu.VMEM((8, round_up(freqs, 8)), f32),
            dma((16,)),
            dma((18,)),
            dma((18,)),
        ],
        compiler_params=pltpu.CompilerParams(
            collective_id=0, has_side_effects=True, vmem_limit_bytes=24 * 2**20
        ),
        name="forward",
    )(*map(keep, (spectrum, adjoint_in, cx, cy, wx, wy, land, ice)),
      *map(keep, (speed.reshape(1, -1), growth.reshape(1, -1), diss.reshape(1, -1), jnp.asarray(trig))))
    return pl.pallas_call(
        transpose_kernel,
        out_shape=shape((rows, cells, bins), f32),
        in_specs=[VMEM] * 4,
        out_specs=HBM,
        scratch_shapes=[
            pltpu.VMEM((cells, bins), f32),
            pltpu.VMEM((rows, cells, bins), f32),
            dma((rows,)),
        ],
        compiler_params=pltpu.CompilerParams(vmem_limit_bytes=16 * 2**20),
        name="transpose",
    )(sens, lat, stats, table)


def solution(mesh):
    grid = P("gx", "gy")
    field = P("gx", "gy", None)
    return jax.shard_map(
        functools.partial(body, mesh.shape["gx"], mesh.shape["gy"]),
        mesh=mesh,
        in_specs=(field, field) + (grid,) * 6 + (P(), P(), P()),
        out_specs=field,
        check_vma=False,
    )
```

```python
import functools
import math

import jax
import jax.numpy as jnp
import numpy as np
from jax import lax
from jax.experimental import pallas as pl
from jax.experimental.pallas import tpu as pltpu
from jax.sharding import PartitionSpec as P

DIRS = 36
LANES = 128
HBM = pl.BlockSpec(memory_space=pltpu.HBM)
VMEM = pl.BlockSpec(memory_space=pltpu.VMEM)


def lane_chunks(bins):
    return [(s, min(LANES, bins - s)) for s in range(0, bins, LANES)]


def up(block, last):
    return jnp.concatenate([block[1:], last], axis=0)


def down(block, first):
    return jnp.concatenate([first, block[:-1]], axis=0)


def spread(cells, stats, table, count):
    for k in range(count):
        turned = table[k][:cells, :]

        def one(i, carry, k=k, turned=turned):
            column = pltpu.roll(turned, LANES - i, axis=1)[:, 0:1]
            stats[k, i] = jnp.broadcast_to(column, (cells, LANES))
            return carry

        lax.fori_loop(1, stats.shape[1], one, 0, unroll=4)
        stats[k, 0] = jnp.broadcast_to(turned[:, 0:1], (cells, LANES))


def kernel(
    nx, ny,
    spectrum, adjoint, cx_h, cy_h, wx_h, wy_h, land_h, ice_h, speed_h, growth_h, diss_h, trig_h,
    done,
    sens, lat_out, stats, table, sp, adj, lat, rim, near_f, near_i, mine_f, mine_i, coeffs, trig, ext, face, turned, flux, work, lat_s, params,
    local_sem, far_send, far_recv,
):
    gx, gy = lax.axis_index("gx"), lax.axis_index("gy")
    rows, cells, bins = adjoint.shape
    east, west = lax.rem(gx + 1, nx), lax.rem(gx + nx - 1, nx)
    has_north, has_south = gy < ny - 1, gy > 0
    chunks = lane_chunks(bins)
    pad = stats.shape[2]

    barrier = pltpu.get_barrier_semaphore()
    for axis, where in (("gx", east), ("gx", west)):
        pl.semaphore_signal(barrier, inc=1, device_id={axis: where}, device_id_type=pl.DeviceIdType.MESH)

    @pl.when(has_north)
    def _():
        pl.semaphore_signal(barrier, inc=1, device_id={"gy": gy + 1}, device_id_type=pl.DeviceIdType.MESH)

    @pl.when(has_south)
    def _():
        pl.semaphore_signal(barrier, inc=1, device_id={"gy": gy - 1}, device_id_type=pl.DeviceIdType.MESH)

    half = rows // 2
    small = []
    cx, cy, wx, wy = (mine_f.at[m] for m in range(4))
    land, ice = (mine_i.at[m] for m in range(2))
    speed, growth, diss = (coeffs.at[m] for m in range(3))
    pairs = (
        (spectrum.at[:, pl.ds(0, 1), :], rim.at[0]), (spectrum.at[:, pl.ds(cells - 1, 1), :], rim.at[1]),
        (cx_h, cx), (cy_h, cy), (land_h, land), (ice_h, ice), (wx_h, wx), (wy_h, wy),
        (speed_h, speed), (growth_h, growth), (diss_h, diss), (trig_h, trig),
    )
    for m, (src, dst) in enumerate(pairs):
        small.append(pltpu.make_async_copy(src, dst, local_sem.at[4 + m]))
    for copy in small:
        copy.start()
    loads = []
    for n, (src, dst, off) in enumerate(((spectrum, sp, 1), (adjoint, adj, 0))):
        for m in range(2):
            loads.append(
                pltpu.make_async_copy(
                    src.at[pl.ds(m * half, half)], dst.at[pl.ds(m * half + off, half)], local_sem.at[2 * n + m]
                )
            )
    for copy in loads:
        copy.start()

    def far(src, dst, n, axis, where):
        return pltpu.make_async_remote_copy(
            src_ref=src, dst_ref=dst, send_sem=far_send.at[n], recv_sem=far_recv.at[n],
            device_id={axis: where}, device_id_type=pl.DeviceIdType.MESH,
        )

    to_east = [
        far(cx_h, near_f.at[0], 0, "gx", east),
        far(land_h, near_i.at[0], 1, "gx", east),
        far(spectrum.at[rows - 1], sp.at[0], 2, "gx", east),
    ]
    to_west = [
        far(cx_h, near_f.at[1], 3, "gx", west),
        far(land_h, near_i.at[1], 4, "gx", west),
        far(spectrum.at[0], sp.at[rows + 1], 5, "gx", west),
    ]
    to_north = [
        far(cy_h, near_f.at[2], 6, "gy", gy + 1),
        far(land_h, near_i.at[2], 7, "gy", gy + 1),
        far(rim.at[1], lat.at[0], 8, "gy", gy + 1),
    ]
    to_south = [
        far(cy_h, near_f.at[3], 9, "gy", gy - 1),
        far(land_h, near_i.at[3], 10, "gy", gy - 1),
        far(rim.at[0], lat.at[1], 11, "gy", gy - 1),
    ]

    @pl.when(jnp.logical_not(has_south))
    def _():
        lat[0] = jnp.zeros(lat.shape[1:], jnp.float32)

    @pl.when(jnp.logical_not(has_north))
    def _():
        lat[1] = jnp.zeros(lat.shape[1:], jnp.float32)

    pl.semaphore_wait(barrier, 2 + has_north.astype(jnp.int32) + has_south.astype(jnp.int32))

    def each_lat(method, first=0, last=3):
        @pl.when(has_north)
        def _():
            for copy in to_north[first:last]:
                getattr(copy, method)()

        @pl.when(has_south)
        def _():
            for copy in to_south[first:last]:
                getattr(copy, method)()

    def lat_arrives(first, last):
        @pl.when(has_south)
        def _():
            for copy in to_north[first:last]:
                copy.wait_recv()

        @pl.when(has_north)
        def _():
            for copy in to_south[first:last]:
                copy.wait_recv()

    for copy in to_east[:2] + to_west[:2]:
        copy.start()
    each_lat("start", 0, 2)
    for copy in to_east[2:] + to_west[2:]:
        copy.start()
    small[0].wait()
    small[1].wait()
    each_lat("start", 2, 3)
    for copy in small[2:]:
        copy.wait()

    freqs = coeffs.shape[2]
    params[...] = jnp.zeros(params.shape, jnp.float32)
    params[0:1, 0:freqs] = speed[...]
    params[1:2, 0:freqs] = growth[...]
    params[2:3, 0:freqs] = diss[...]
    spots = lax.rem(lax.broadcasted_iota(jnp.int32, (params.shape[1], bins), 1), freqs)
    hot = (spots == lax.broadcasted_iota(jnp.int32, (params.shape[1], bins), 0)).astype(jnp.float32)
    by_bin = jnp.dot(params[...], hot, precision=lax.Precision.HIGHEST, preferred_element_type=jnp.float32)
    cosine, sine = trig[0:1], trig[1:2]
    table[0:1] = by_bin[0:1] * cosine
    table[1:2] = by_bin[0:1] * sine
    table[2:3] = by_bin[1:2] * cosine
    table[3:4] = by_bin[1:2] * sine
    table[4:5] = by_bin[2:3]

    for copy in to_east[:2] + to_west[:2]:
        copy.wait_recv()
    lat_arrives(0, 2)
    ext[...] = jnp.zeros(ext.shape, jnp.float32)
    sea_of = lambda mask: (1 - mask).astype(jnp.float32)
    ext[0, 0:1, 0:cells] = near_f[0, rows - 1 : rows]
    ext[0, 1 : rows + 1, 0:cells] = cx[...]
    ext[0, rows + 1 : rows + 2, 0:cells] = near_f[1, 0:1]
    ext[1, 0:1, 0:cells] = sea_of(near_i[0, rows - 1 : rows])
    ext[1, 1 : rows + 1, 0:cells] = sea_of(land[...])
    ext[1, rows + 1 : rows + 2, 0:cells] = sea_of(near_i[1, 0:1])
    ext[2, 0:rows, 0:cells] = cy[...]
    ext[3, 0:rows, 0:cells] = sea_of(land[...])
    ext[4, 0:rows, 0:cells] = near_f[2]
    ext[5, 0:rows, 0:cells] = sea_of(near_i[2])
    ext[6, 0:rows, 0:cells] = near_f[3]
    ext[7, 0:rows, 0:cells] = sea_of(near_i[3])
    face[...] = jnp.zeros(face.shape, jnp.float32)
    opened = ext[1, 0 : rows + 1] * ext[1, 1 : rows + 2]
    face[0, 0 : rows + 1] = opened
    face[1, 0 : rows + 1] = opened * (0.5 * (ext[0, 0 : rows + 1] + ext[0, 1 : rows + 2]))
    tall = ext.shape[1]
    lane = lax.broadcasted_iota(jnp.int32, (tall, LANES), 1)

    def pair(own, south, north):
        mine = jnp.where(lane == cells, pltpu.roll(own, cells, axis=1), own)
        other = jnp.where(lane == cells - 1, pltpu.roll(north, cells - 1, axis=1), pltpu.roll(own, LANES - 1, axis=1))
        other = jnp.where(lane == cells, pltpu.roll(south, 1, axis=1), other)
        return mine, other

    sea_a, sea_b = pair(ext[3], ext[5], ext[7])
    cy_a, cy_b = pair(ext[2], ext[4], ext[6])
    closed = jnp.logical_or(
        jnp.logical_and(lane == cells, jnp.logical_not(has_south)),
        jnp.logical_and(lane == cells - 1, jnp.logical_not(has_north)),
    )
    opened = sea_a * sea_b
    face[2, 0:tall] = jnp.where(closed, 0.0, opened)
    face[3, 0:tall] = jnp.where(closed, 0.0, opened * (0.5 * (cy_a + cy_b)))
    ice_free = sea_of(ice[...])
    face[4, 0:rows, 0:cells] = wx[...] * ice_free
    face[5, 0:rows, 0:cells] = wy[...] * ice_free
    face[6, 0:rows, 0:cells] = sea_of(land[...])
    for k in range(7):
        turned[k] = face[k].T
    spread(pad, stats, turned, 7)

    for copy in loads:
        copy.wait()
    lat_arrives(2, 3)

    def lon_flux(f, s, w):
        courant = stats[0, f, 0:cells, 0:w] * table[0:1, s : s + w] + stats[1, f, 0:cells, 0:w]
        return courant * jnp.where(courant > 0, sp[f, :, s : s + w], sp[f + 1, :, s : s + w])

    lon_send = [
        far(sens.at[rows], sens.at[0], 12, "gx", east),
        far(sens.at[1], sens.at[rows + 1], 13, "gx", west),
    ]
    lat_north = [far(lat_s.at[1, pl.ds(m * half, half)], lat_out.at[0, pl.ds(m * half, half)], 14 + m, "gy", gy + 1) for m in range(2)]
    lat_south = [far(lat_s.at[0, pl.ds(m * half, half)], lat_out.at[1, pl.ds(m * half, half)], 16 + m, "gy", gy - 1) for m in range(2)]

    def lat_send(m):
        @pl.when(has_north)
        def _():
            lat_north[m].start()

        @pl.when(has_south)
        def _():
            lat_south[m].start()

    def lat_done(m):
        @pl.when(has_north)
        def _():
            lat_south[m].wait_recv()

        @pl.when(has_south)
        def _():
            lat_north[m].wait_recv()

    early = rows // 3

    def row(k, carry):
        i = jnp.where(k < early, k + 1, jnp.where(k == early, 0, jnp.where(k == early + 1, rows - 1, k - 1)))

        @pl.when(k == early)
        def _():
            for copy in to_east[2:] + to_west[2:]:
                copy.wait_recv()

        @pl.when(jnp.logical_or(k == 0, jnp.logical_and(k >= early, k < early + 3)))
        def _():
            for s, w in chunks:
                flux[:, s : s + w] = lon_flux(i, s, w)

        @pl.when(k == early + 3)
        def _():
            for copy in lon_send:
                copy.start()

        @pl.when(k == half + 2)
        def _():
            lat_send(0)

        energy = jnp.zeros((cells, 1), jnp.float32)
        total = jnp.zeros((cells, LANES), jnp.float32)
        for s, w in chunks:
            own = sp[i + 1, :, s : s + w]
            fx = lon_flux(i + 1, s, w)
            fx_low = flux[:, s : s + w]
            sin_row = table[1:2, s : s + w]
            courant = stats[2, i, 0:cells, 0:w] * sin_row + stats[3, i, 0:cells, 0:w]
            fy = courant * jnp.where(courant > 0, own, up(own, lat[1, i, :, s : s + w]))
            low = stats[2, i, cells : cells + 1, 0:w] * sin_row + stats[3, i, cells : cells + 1, 0:w]
            fy_low = down(fy, low * jnp.where(low > 0, lat[0, i, :, s : s + w], own[0:1]))
            advected = own - (fx - fx_low) - (fy - fy_low)
            flux[:, s : s + w] = fx
            work[:, s : s + w] = advected
            if w == LANES:
                total = total + advected
            else:
                energy = energy + jnp.sum(advected, axis=1, keepdims=True)
        energy = (energy + jnp.sum(total, axis=1, keepdims=True)) * (1.0 / bins)
        energy = jnp.broadcast_to(energy, (cells, LANES))
        coupling = jnp.zeros((cells, 1), jnp.float32)
        total = jnp.zeros((cells, LANES), jnp.float32)
        for s, w in chunks:
            advected = work[:, s : s + w]
            blow = stats[4, i, 0:cells, 0:w] * table[2:3, s : s + w] + stats[5, i, 0:cells, 0:w] * table[3:4, s : s + w]
            gain = 1.0 + jnp.maximum(blow, 0.0)
            scaled = table[4:5, s : s + w] * advected
            damp = 1.0 + energy[:, 0:w] * scaled
            weighted = adj[i, :, s : s + w] * gain / (damp * damp)
            sens[i + 1, :, s : s + w] = weighted
            term = weighted * scaled * advected
            if w == LANES:
                total = total + term
            else:
                coupling = coupling + jnp.sum(term, axis=1, keepdims=True)
        coupling = (coupling + jnp.sum(total, axis=1, keepdims=True)) * (1.0 / bins)
        coupling = jnp.broadcast_to(coupling, (cells, LANES))
        for s, w in chunks:
            value = stats[6, i, 0:cells, 0:w] * (sens[i + 1, :, s : s + w] - coupling[:, 0:w])
            sens[i + 1, :, s : s + w] = value
            lat_s[0, i, :, s : s + w] = value[0:1]
            lat_s[1, i, :, s : s + w] = value[cells - 1 : cells]

        return carry

    lax.fori_loop(0, rows, row, 0)
    lat_send(1)

    fill = [pltpu.make_async_copy(lat.at[m], lat_out.at[m], local_sem.at[m]) for m in range(2)]
    for m, there in ((0, has_south), (1, has_north)):
        @pl.when(jnp.logical_not(there))
        def _(m=m):
            fill[m].start()

    for m, there in ((0, has_south), (1, has_north)):
        @pl.when(jnp.logical_not(there))
        def _(m=m):
            fill[m].wait()

    lat_done(0)

    def lon_face(f, s, w):
        return stats[0, f, 0:cells, 0:w] * table[0:1, s : s + w] + stats[1, f, 0:cells, 0:w]

    def back(k, carry):
        i = jnp.where(k < rows - 2, k + 1, jnp.where(k == rows - 2, 0, rows - 1))

        @pl.when(k == half - 1)
        def _():
            lat_done(1)

        @pl.when(k == rows - 2)
        def _():
            for copy in lon_send:
                copy.wait_recv()

        @pl.when(jnp.logical_or(k == 0, k >= rows - 2))
        def _():
            for s, w in chunks:
                flux[:, s : s + w] = jnp.minimum(lon_face(i, s, w), 0.0) * (
                    sens[i + 1, :, s : s + w] - sens[i, :, s : s + w]
                )

        for s, w in chunks:
            own = sens[i + 1, :, s : s + w]
            step = sens[i + 2, :, s : s + w] - own
            courant = lon_face(i + 1, s, w)
            value = own + flux[:, s : s + w] + jnp.maximum(courant, 0.0) * step
            flux[:, s : s + w] = jnp.minimum(courant, 0.0) * step
            sin_row = table[1:2, s : s + w]
            courant = stats[2, i, 0:cells, 0:w] * sin_row + stats[3, i, 0:cells, 0:w]
            step = up(own, lat_out[1, i, :, s : s + w]) - own
            value = value + jnp.maximum(courant, 0.0) * step
            low = stats[2, i, cells : cells + 1, 0:w] * sin_row + stats[3, i, cells : cells + 1, 0:w]
            low = jnp.minimum(low, 0.0) * (own[0:1] - lat_out[0, i, :, s : s + w])
            done[i, :, s : s + w] = value + down(jnp.minimum(courant, 0.0) * step, low)
        return carry

    lax.fori_loop(0, rows, back, 0)

    for copy in to_east + to_west + lon_send:
        copy.wait_send()
    each_lat("wait_send")

    @pl.when(has_north)
    def _():
        for copy in lat_north:
            copy.wait_send()

    @pl.when(has_south)
    def _():
        for copy in lat_south:
            copy.wait_send()


def keep(array):
    return pltpu.with_memory_space_constraint(array, pltpu.HBM)


def round_up(value, step):
    return (value + step - 1) // step * step


def body(nx, ny, spectrum, adjoint_in, cx, cy, wx, wy, land, ice, speed, growth, diss):
    rows, cells, bins = spectrum.shape
    freqs = speed.shape[0]
    angles = 2.0 * math.pi / DIRS * (np.arange(DIRS) + 0.5)
    trig = np.stack([np.repeat(np.cos(angles), freqs), np.repeat(np.sin(angles), freqs)]).astype(np.float32)
    pad = round_up(cells + 1, 8)
    tall = round_up(rows + 2, 8)
    f32 = jnp.float32
    dma = pltpu.SemaphoreType.DMA
    shape = jax.ShapeDtypeStruct
    return pl.pallas_call(
        functools.partial(kernel, nx, ny),
        out_shape=shape((rows, cells, bins), f32),
        in_specs=[HBM] * 12,
        out_specs=VMEM,
        scratch_shapes=[
            pltpu.VMEM((rows + 2, cells, bins), f32),
            pltpu.VMEM((2, rows, 1, bins), f32),
            pltpu.VMEM((7, rows + 1, pad, LANES), f32),
            pltpu.VMEM((8, bins), f32),
            pltpu.VMEM((rows + 2, cells, bins), f32),
            pltpu.VMEM((rows, cells, bins), f32),
            pltpu.VMEM((2, rows, 1, bins), f32),
            pltpu.VMEM((2, rows, 1, bins), f32),
            pltpu.VMEM((4, rows, cells), f32),
            pltpu.VMEM((4, rows, cells), jnp.int32),
            pltpu.VMEM((4, rows, cells), f32),
            pltpu.VMEM((2, rows, cells), jnp.int32),
            pltpu.VMEM((3, 1, freqs), f32),
            pltpu.VMEM((2, bins), f32),
            pltpu.VMEM((8, tall, LANES), f32),
            pltpu.VMEM((7, LANES, LANES), f32),
            pltpu.VMEM((7, LANES, LANES), f32),
            pltpu.VMEM((cells, bins), f32),
            pltpu.VMEM((cells, bins), f32),
            pltpu.VMEM((2, rows, 1, bins), f32),
            pltpu.VMEM((8, round_up(freqs, 8)), f32),
            dma((16,)),
            dma((18,)),
            dma((18,)),
        ],
        compiler_params=pltpu.CompilerParams(
            collective_id=0, has_side_effects=True, vmem_limit_bytes=36 * 2**20
        ),
        name="step",
    )(*map(keep, (spectrum, adjoint_in, cx, cy, wx, wy, land, ice)),
      *map(keep, (speed.reshape(1, -1), growth.reshape(1, -1), diss.reshape(1, -1), jnp.asarray(trig))))


def solution(mesh):
    grid = P("gx", "gy")
    field = P("gx", "gy", None)
    return jax.shard_map(
        functools.partial(body, mesh.shape["gx"], mesh.shape["gy"]),
        mesh=mesh,
        in_specs=(field, field) + (grid,) * 6 + (P(), P(), P()),
        out_specs=field,
        check_vma=False,
    )
```

```python
import functools
import math

import jax
import jax.numpy as jnp
import numpy as np
from jax import lax
from jax.experimental import pallas as pl
from jax.experimental.pallas import tpu as pltpu
from jax.sharding import PartitionSpec as P

DIRS = 36
LANES = 128
HBM = pl.BlockSpec(memory_space=pltpu.HBM)
VMEM = pl.BlockSpec(memory_space=pltpu.VMEM)


def lane_chunks(bins):
    return [(s, min(LANES, bins - s)) for s in range(0, bins, LANES)]


def up(block, last):
    return jnp.concatenate([block[1:], last], axis=0)


def down(block, first):
    return jnp.concatenate([first, block[:-1]], axis=0)


def spread(stats, turned, first, last):
    columns, pad = stats.shape[1:3]

    def one(k, carry):
        for i in range(columns):
            stats[k, i] = jnp.broadcast_to(turned[k, 0:pad, i : i + 1], (pad, LANES))
        return carry

    lax.fori_loop(first, last, one, 0)


def kernel(
    nx, ny,
    spectrum, adjoint, cx_h, cy_h, wx_h, wy_h, land_h, ice_h, speed_h, growth_h, diss_h, trig_h,
    done,
    sens, lat_out, stats, table, sp, adj, lat, rim, near_f, near_i, mine_f, mine_i, coeffs, trig, ext, face, turned, flux, work, lat_s, params,
    local_sem, far_send, far_recv,
):
    gx, gy = lax.axis_index("gx"), lax.axis_index("gy")
    rows, cells, bins = adjoint.shape
    east, west = lax.rem(gx + 1, nx), lax.rem(gx + nx - 1, nx)
    has_north, has_south = gy < ny - 1, gy > 0
    chunks = lane_chunks(bins)
    pad = stats.shape[2]

    barrier = pltpu.get_barrier_semaphore()
    for axis, where in (("gx", east), ("gx", west)):
        pl.semaphore_signal(barrier, inc=1, device_id={axis: where}, device_id_type=pl.DeviceIdType.MESH)

    @pl.when(has_north)
    def _():
        pl.semaphore_signal(barrier, inc=1, device_id={"gy": gy + 1}, device_id_type=pl.DeviceIdType.MESH)

    @pl.when(has_south)
    def _():
        pl.semaphore_signal(barrier, inc=1, device_id={"gy": gy - 1}, device_id_type=pl.DeviceIdType.MESH)

    half = rows // 2
    small = []
    cx, cy, wx, wy = (mine_f.at[m] for m in range(4))
    land, ice = (mine_i.at[m] for m in range(2))
    speed, growth, diss = (coeffs.at[m] for m in range(3))
    pairs = (
        (spectrum.at[:, pl.ds(0, 1), :], rim.at[0]), (spectrum.at[:, pl.ds(cells - 1, 1), :], rim.at[1]),
        (cx_h, cx), (cy_h, cy), (land_h, land), (ice_h, ice), (wx_h, wx), (wy_h, wy),
        (speed_h, speed), (growth_h, growth), (diss_h, diss), (trig_h, trig),
    )
    for m, (src, dst) in enumerate(pairs):
        small.append(pltpu.make_async_copy(src, dst, local_sem.at[4 + m]))
    for copy in small:
        copy.start()
    loads = []
    for n, (src, dst, off) in enumerate(((spectrum, sp, 1), (adjoint, adj, 0))):
        for m in range(2):
            loads.append(
                pltpu.make_async_copy(
                    src.at[pl.ds(m * half, half)], dst.at[pl.ds(m * half + off, half)], local_sem.at[2 * n + m]
                )
            )
    for copy in loads[:2]:
        copy.start()

    def far(src, dst, n, axis, where):
        return pltpu.make_async_remote_copy(
            src_ref=src, dst_ref=dst, send_sem=far_send.at[n], recv_sem=far_recv.at[n],
            device_id={axis: where}, device_id_type=pl.DeviceIdType.MESH,
        )

    to_east = [
        far(cx_h, near_f.at[0], 0, "gx", east),
        far(land_h, near_i.at[0], 1, "gx", east),
        far(spectrum.at[rows - 1], sp.at[0], 2, "gx", east),
    ]
    to_west = [
        far(cx_h, near_f.at[1], 3, "gx", west),
        far(land_h, near_i.at[1], 4, "gx", west),
        far(spectrum.at[0], sp.at[rows + 1], 5, "gx", west),
    ]
    to_north = [
        far(cy_h, near_f.at[2], 6, "gy", gy + 1),
        far(land_h, near_i.at[2], 7, "gy", gy + 1),
        far(rim.at[1], lat.at[0], 8, "gy", gy + 1),
    ]
    to_south = [
        far(cy_h, near_f.at[3], 9, "gy", gy - 1),
        far(land_h, near_i.at[3], 10, "gy", gy - 1),
        far(rim.at[0], lat.at[1], 11, "gy", gy - 1),
    ]

    @pl.when(jnp.logical_not(has_south))
    def _():
        lat[0] = jnp.zeros(lat.shape[1:], jnp.float32)

    @pl.when(jnp.logical_not(has_north))
    def _():
        lat[1] = jnp.zeros(lat.shape[1:], jnp.float32)

    pl.semaphore_wait(barrier, 2 + has_north.astype(jnp.int32) + has_south.astype(jnp.int32))

    def each_lat(method, first=0, last=3):
        @pl.when(has_north)
        def _():
            for copy in to_north[first:last]:
                getattr(copy, method)()

        @pl.when(has_south)
        def _():
            for copy in to_south[first:last]:
                getattr(copy, method)()

    def lat_arrives(first, last):
        @pl.when(has_south)
        def _():
            for copy in to_north[first:last]:
                copy.wait_recv()

        @pl.when(has_north)
        def _():
            for copy in to_south[first:last]:
                copy.wait_recv()

    for copy in to_east[:2] + to_west[:2]:
        copy.start()
    each_lat("start", 0, 2)
    for copy in to_east[2:] + to_west[2:]:
        copy.start()
    small[0].wait()
    small[1].wait()
    each_lat("start", 2, 3)
    for copy in loads[2:]:
        copy.start()
    for copy in small[2:]:
        copy.wait()

    freqs = coeffs.shape[2]
    params[...] = jnp.zeros(params.shape, jnp.float32)
    params[0:1, 0:freqs] = speed[...]
    params[1:2, 0:freqs] = growth[...]
    params[2:3, 0:freqs] = diss[...]
    spots = lax.rem(lax.broadcasted_iota(jnp.int32, (params.shape[1], bins), 1), freqs)
    hot = (spots == lax.broadcasted_iota(jnp.int32, (params.shape[1], bins), 0)).astype(jnp.float32)
    by_bin = jnp.dot(params[...], hot, precision=lax.Precision.HIGHEST, preferred_element_type=jnp.float32)
    cosine, sine = trig[0:1], trig[1:2]
    table[0:1] = by_bin[0:1] * cosine
    table[1:2] = by_bin[0:1] * sine
    table[2:3] = by_bin[1:2] * cosine
    table[3:4] = by_bin[1:2] * sine
    table[4:5] = by_bin[2:3]

    sea_of = lambda mask: (1 - mask).astype(jnp.float32)
    face[...] = jnp.zeros(face.shape, jnp.float32)
    ice_free = sea_of(ice[...])
    face[4, 0:rows, 0:cells] = wx[...] * ice_free
    face[5, 0:rows, 0:cells] = wy[...] * ice_free
    face[6, 0:rows, 0:cells] = sea_of(land[...])
    for k in range(4, 7):
        turned[k] = face[k].T
    spread(stats, turned, 4, 7)
    for copy in to_east[:2] + to_west[:2]:
        copy.wait_recv()
    lat_arrives(0, 2)
    ext[...] = jnp.zeros(ext.shape, jnp.float32)
    ext[0, 0:1, 0:cells] = near_f[0, rows - 1 : rows]
    ext[0, 1 : rows + 1, 0:cells] = cx[...]
    ext[0, rows + 1 : rows + 2, 0:cells] = near_f[1, 0:1]
    ext[1, 0:1, 0:cells] = sea_of(near_i[0, rows - 1 : rows])
    ext[1, 1 : rows + 1, 0:cells] = sea_of(land[...])
    ext[1, rows + 1 : rows + 2, 0:cells] = sea_of(near_i[1, 0:1])
    ext[2, 0:rows, 0:cells] = cy[...]
    ext[3, 0:rows, 0:cells] = sea_of(land[...])
    ext[4, 0:rows, 0:cells] = near_f[2]
    ext[5, 0:rows, 0:cells] = sea_of(near_i[2])
    ext[6, 0:rows, 0:cells] = near_f[3]
    ext[7, 0:rows, 0:cells] = sea_of(near_i[3])
    opened = ext[1, 0 : rows + 1] * ext[1, 1 : rows + 2]
    face[0, 0 : rows + 1] = opened
    face[1, 0 : rows + 1] = opened * (0.5 * (ext[0, 0 : rows + 1] + ext[0, 1 : rows + 2]))
    tall = ext.shape[1]
    lane = lax.broadcasted_iota(jnp.int32, (tall, LANES), 1)

    def pair(own, south, north):
        mine = jnp.where(lane == cells, pltpu.roll(own, cells, axis=1), own)
        other = jnp.where(lane == cells - 1, pltpu.roll(north, cells - 1, axis=1), pltpu.roll(own, LANES - 1, axis=1))
        other = jnp.where(lane == cells, pltpu.roll(south, 1, axis=1), other)
        return mine, other

    sea_a, sea_b = pair(ext[3], ext[5], ext[7])
    cy_a, cy_b = pair(ext[2], ext[4], ext[6])
    closed = jnp.logical_or(
        jnp.logical_and(lane == cells, jnp.logical_not(has_south)),
        jnp.logical_and(lane == cells - 1, jnp.logical_not(has_north)),
    )
    opened = sea_a * sea_b
    face[2, 0:tall] = jnp.where(closed, 0.0, opened)
    face[3, 0:tall] = jnp.where(closed, 0.0, opened * (0.5 * (cy_a + cy_b)))
    for k in range(4):
        turned[k] = face[k].T
    spread(stats, turned, 0, 4)

    for copy in loads:
        copy.wait()
    lat_arrives(2, 3)

    def lon_flux(f, s, w):
        courant = stats[0, f, 0:cells, 0:w] * table[0:1, s : s + w] + stats[1, f, 0:cells, 0:w]
        return courant * jnp.where(courant > 0, sp[f, :, s : s + w], sp[f + 1, :, s : s + w])

    lon_send = [
        far(sens.at[rows], sens.at[0], 12, "gx", east),
        far(sens.at[1], sens.at[rows + 1], 13, "gx", west),
    ]
    lat_north = [far(lat_s.at[1, pl.ds(m * half, half)], lat_out.at[0, pl.ds(m * half, half)], 14 + m, "gy", gy + 1) for m in range(2)]
    lat_south = [far(lat_s.at[0, pl.ds(m * half, half)], lat_out.at[1, pl.ds(m * half, half)], 16 + m, "gy", gy - 1) for m in range(2)]

    def lat_send(m):
        @pl.when(has_north)
        def _():
            lat_north[m].start()

        @pl.when(has_south)
        def _():
            lat_south[m].start()

    def lat_done(m):
        @pl.when(has_north)
        def _():
            lat_south[m].wait_recv()

        @pl.when(has_south)
        def _():
            lat_north[m].wait_recv()

    early = rows // 3

    def row(k, carry):
        i = jnp.where(k < early, k + 1, jnp.where(k == early, 0, jnp.where(k == early + 1, rows - 1, k - 1)))

        @pl.when(k == early)
        def _():
            for copy in to_east[2:] + to_west[2:]:
                copy.wait_recv()

        @pl.when(jnp.logical_or(k == 0, jnp.logical_and(k >= early, k < early + 3)))
        def _():
            for s, w in chunks:
                flux[:, s : s + w] = lon_flux(i, s, w)

        @pl.when(k == early + 3)
        def _():
            for copy in lon_send:
                copy.start()

        @pl.when(k == half + 2)
        def _():
            lat_send(0)

        energy = jnp.zeros((cells, 1), jnp.float32)
        total = jnp.zeros((cells, LANES), jnp.float32)
        for s, w in chunks:
            own = sp[i + 1, :, s : s + w]
            fx = lon_flux(i + 1, s, w)
            fx_low = flux[:, s : s + w]
            sin_row = table[1:2, s : s + w]
            courant = stats[2, i, 0:cells, 0:w] * sin_row + stats[3, i, 0:cells, 0:w]
            fy = courant * jnp.where(courant > 0, own, up(own, lat[1, i, :, s : s + w]))
            low = stats[2, i, cells : cells + 1, 0:w] * sin_row + stats[3, i, cells : cells + 1, 0:w]
            fy_low = down(fy, low * jnp.where(low > 0, lat[0, i, :, s : s + w], own[0:1]))
            advected = own - (fx - fx_low) - (fy - fy_low)
            flux[:, s : s + w] = fx
            work[:, s : s + w] = advected
            if w == LANES:
                total = total + advected
            else:
                energy = energy + jnp.sum(advected, axis=1, keepdims=True)
        energy = (energy + jnp.sum(total, axis=1, keepdims=True)) * (1.0 / bins)
        energy = jnp.broadcast_to(energy, (cells, LANES))
        coupling = jnp.zeros((cells, 1), jnp.float32)
        total = jnp.zeros((cells, LANES), jnp.float32)
        for s, w in chunks:
            advected = work[:, s : s + w]
            blow = stats[4, i, 0:cells, 0:w] * table[2:3, s : s + w] + stats[5, i, 0:cells, 0:w] * table[3:4, s : s + w]
            gain = 1.0 + jnp.maximum(blow, 0.0)
            scaled = table[4:5, s : s + w] * advected
            damp = 1.0 + energy[:, 0:w] * scaled
            weighted = adj[i, :, s : s + w] * gain / (damp * damp)
            sens[i + 1, :, s : s + w] = weighted
            term = weighted * scaled * advected
            if w == LANES:
                total = total + term
            else:
                coupling = coupling + jnp.sum(term, axis=1, keepdims=True)
        coupling = (coupling + jnp.sum(total, axis=1, keepdims=True)) * (1.0 / bins)
        coupling = jnp.broadcast_to(coupling, (cells, LANES))
        for s, w in chunks:
            value = stats[6, i, 0:cells, 0:w] * (sens[i + 1, :, s : s + w] - coupling[:, 0:w])
            sens[i + 1, :, s : s + w] = value
            lat_s[0, i, :, s : s + w] = value[0:1]
            lat_s[1, i, :, s : s + w] = value[cells - 1 : cells]

        return carry

    lax.fori_loop(0, rows, row, 0)
    lat_send(1)

    fill = [pltpu.make_async_copy(lat.at[m], lat_out.at[m], local_sem.at[m]) for m in range(2)]
    for m, there in ((0, has_south), (1, has_north)):
        @pl.when(jnp.logical_not(there))
        def _(m=m):
            fill[m].start()

    for m, there in ((0, has_south), (1, has_north)):
        @pl.when(jnp.logical_not(there))
        def _(m=m):
            fill[m].wait()

    lat_done(0)

    def lon_face(f, s, w):
        return stats[0, f, 0:cells, 0:w] * table[0:1, s : s + w] + stats[1, f, 0:cells, 0:w]

    def back(k, carry):
        i = jnp.where(k < rows - 2, k + 1, jnp.where(k == rows - 2, 0, rows - 1))

        @pl.when(k == half - 1)
        def _():
            lat_done(1)

        @pl.when(k == rows - 2)
        def _():
            for copy in lon_send:
                copy.wait_recv()

        @pl.when(jnp.logical_or(k == 0, k >= rows - 2))
        def _():
            for s, w in chunks:
                flux[:, s : s + w] = jnp.minimum(lon_face(i, s, w), 0.0) * (
                    sens[i + 1, :, s : s + w] - sens[i, :, s : s + w]
                )

        for s, w in chunks:
            own = sens[i + 1, :, s : s + w]
            step = sens[i + 2, :, s : s + w] - own
            courant = lon_face(i + 1, s, w)
            value = own + flux[:, s : s + w] + jnp.maximum(courant, 0.0) * step
            flux[:, s : s + w] = jnp.minimum(courant, 0.0) * step
            sin_row = table[1:2, s : s + w]
            courant = stats[2, i, 0:cells, 0:w] * sin_row + stats[3, i, 0:cells, 0:w]
            step = up(own, lat_out[1, i, :, s : s + w]) - own
            value = value + jnp.maximum(courant, 0.0) * step
            low = stats[2, i, cells : cells + 1, 0:w] * sin_row + stats[3, i, cells : cells + 1, 0:w]
            low = jnp.minimum(low, 0.0) * (own[0:1] - lat_out[0, i, :, s : s + w])
            done[i, :, s : s + w] = value + down(jnp.minimum(courant, 0.0) * step, low)
        return carry

    lax.fori_loop(0, rows, back, 0)

    for copy in to_east + to_west + lon_send:
        copy.wait_send()
    each_lat("wait_send")

    @pl.when(has_north)
    def _():
        for copy in lat_north:
            copy.wait_send()

    @pl.when(has_south)
    def _():
        for copy in lat_south:
            copy.wait_send()


def keep(array):
    return pltpu.with_memory_space_constraint(array, pltpu.HBM)


def round_up(value, step):
    return (value + step - 1) // step * step


def body(nx, ny, spectrum, adjoint_in, cx, cy, wx, wy, land, ice, speed, growth, diss):
    rows, cells, bins = spectrum.shape
    freqs = speed.shape[0]
    angles = 2.0 * math.pi / DIRS * (np.arange(DIRS) + 0.5)
    trig = np.stack([np.repeat(np.cos(angles), freqs), np.repeat(np.sin(angles), freqs)]).astype(np.float32)
    pad = round_up(cells + 1, 8)
    tall = round_up(rows + 2, 8)
    f32 = jnp.float32
    dma = pltpu.SemaphoreType.DMA
    shape = jax.ShapeDtypeStruct
    return pl.pallas_call(
        functools.partial(kernel, nx, ny),
        out_shape=shape((rows, cells, bins), f32),
        in_specs=[HBM] * 12,
        out_specs=VMEM,
        scratch_shapes=[
            pltpu.VMEM((rows + 2, cells, bins), f32),
            pltpu.VMEM((2, rows, 1, bins), f32),
            pltpu.VMEM((7, rows + 1, pad, LANES), f32),
            pltpu.VMEM((8, bins), f32),
            pltpu.VMEM((rows + 2, cells, bins), f32),
            pltpu.VMEM((rows, cells, bins), f32),
            pltpu.VMEM((2, rows, 1, bins), f32),
            pltpu.VMEM((2, rows, 1, bins), f32),
            pltpu.VMEM((4, rows, cells), f32),
            pltpu.VMEM((4, rows, cells), jnp.int32),
            pltpu.VMEM((4, rows, cells), f32),
            pltpu.VMEM((2, rows, cells), jnp.int32),
            pltpu.VMEM((3, 1, freqs), f32),
            pltpu.VMEM((2, bins), f32),
            pltpu.VMEM((8, tall, LANES), f32),
            pltpu.VMEM((7, LANES, LANES), f32),
            pltpu.VMEM((7, LANES, LANES), f32),
            pltpu.VMEM((cells, bins), f32),
            pltpu.VMEM((cells, bins), f32),
            pltpu.VMEM((2, rows, 1, bins), f32),
            pltpu.VMEM((8, round_up(freqs, 8)), f32),
            dma((16,)),
            dma((18,)),
            dma((18,)),
        ],
        compiler_params=pltpu.CompilerParams(
            collective_id=0, has_side_effects=True, vmem_limit_bytes=36 * 2**20
        ),
        name="step",
    )(*map(keep, (spectrum, adjoint_in, cx, cy, wx, wy, land, ice)),
      *map(keep, (speed.reshape(1, -1), growth.reshape(1, -1), diss.reshape(1, -1), jnp.asarray(trig))))


def solution(mesh):
    grid = P("gx", "gy")
    field = P("gx", "gy", None)
    return jax.shard_map(
        functools.partial(body, mesh.shape["gx"], mesh.shape["gy"]),
        mesh=mesh,
        in_specs=(field, field) + (grid,) * 6 + (P(), P(), P()),
        out_specs=field,
        check_vma=False,
    )
```
